256 devices in a mesh: vert: 64 (over x, z, core), af: 4 (over y).
Axes of the slice: x: 4, y: 4, z: 8, core: 2. Of those that a mesh axis runs over, the one named last changes fastest.
Arguments:
- features_t: bfloat16 [128, 32768], P('af', 'vert'), may hold values from -24 to 24
- weight: bfloat16 [128, 256], P('af'), may hold values from -1 to 1
- bias: float32 [256], P('af'), may hold values from -3 to 3
- self_mask: int32 [64, 512, 512], P('vert'), may hold values 0 or 1
- halo_mask: int32 [64, 6, 512, 256], P('vert'), may hold values 0 or 1
- block_src: int32 [64, 6], P('vert'), may hold values from -1 to 63, as said below
- halo_rows: int32 [64, 6, 256], P('vert'), may hold values from 0 to 511, as said below
- outside_degree: int32 [32768], P('vert'), may hold values from 0 to 47
Outputs:
- output_t: bfloat16 [256, 32768], P('af', 'vert')
The draws below stay inside these ranges and needn't reach their ends.
Inputs may be any that keep to these rules, and one draw needn't show every extreme that they name: `block_src`: the live sources of a row are distinct partitions other than the row's own; empty slots (-1) come after the live ones; every row has at least one live slot and some row has all 6. `halo_rows`: the entries of one slot are distinct.
All inputs are finite; a program needn't handle non-finite values. No bound on the sum of `self_mask` or of `halo_mask` on one device may be relied on, other than what follows from the above.
Results may differ from the reference program's by a relative error of at most 0.0054.
Values may be sent and summed in bfloat16 or wider, within the bound.
No kernel may reach another device: no remote copies, remote signals or barrier semaphores. Data moves between devices by JAX's collectives and lax.ppermute only.
A program may use at most 64 MiB of HBM per device.

```python
import jax
import jax.numpy as jnp
from jax import lax

F_IN = 128
F_OUT = 256
BLOCK = 512
NB = 6
HALO = 256
VERTICES = 32768
N_VERT = 64


def shuffled_offsets(one_key):
    return jax.random.permutation(one_key, N_VERT - 1)[:NB]


def shuffled_rows(one_key):
    return jax.random.permutation(one_key, BLOCK)[:HALO]


def draw_block_src(key, part):
    keys = jax.random.split(jax.random.fold_in(key, 11), N_VERT)
    offsets = jax.vmap(shuffled_offsets)(keys) + 1
    sources = (jnp.arange(N_VERT)[:, None] + offsets) % N_VERT
    live_count = jax.random.randint(jax.random.fold_in(key, 12), (N_VERT,), 1, NB + 1)
    full_row = jax.random.randint(jax.random.fold_in(key, 13), (), 0, N_VERT)
    live_count = jnp.where(jnp.arange(N_VERT) == full_row, NB, live_count)
    return jnp.where(jnp.arange(NB)[None, :] < live_count[:, None], sources, -1).astype(jnp.int32)


def draw_halo_rows(key, part):
    keys = jax.random.split(jax.random.fold_in(key, 21), N_VERT * NB)
    picked = jax.vmap(shuffled_rows)(keys)
    return picked.reshape(N_VERT, NB, HALO).astype(jnp.int32)


def with_ends(entries, key, smallest, top_value):
    longest = entries.shape.index(max(entries.shape))
    spots = []
    for shift in (0, 1):
        where = [jax.random.randint(jax.random.fold_in(key, axis), (), 0, length) for axis, length in enumerate(entries.shape)]
        where[longest] = (where[longest] + shift) % entries.shape[longest]
        spots.append(tuple(where))
    return entries.at[spots[0]].set(smallest).at[spots[1]].set(top_value)


def shard_levels(rng, dims, cuts, smallest, largest):
    factor_of, own = 1.0, jax.random.fold_in(rng, 6)
    for position, parts in cuts:
        heights = jnp.exp(jax.random.uniform(jax.random.fold_in(own, position), (parts,), jnp.float32, smallest / len(cuts), largest / len(cuts)))
        factor_of = factor_of * jnp.repeat(heights, dims[position] // parts).reshape([-1 if axis == position else 1 for axis in range(len(dims))])
    return factor_of


def noise(own_key, dims, width, bound, cuts=(), held_as=jnp.bfloat16):
    drawn = jax.random.normal(own_key, dims, jnp.float32) * width
    if len(cuts) > 0:
        drawn = shard_levels(own_key, dims, cuts, -0.22, 0.18) * drawn
    return jnp.clip(drawn, min=-bound, max=bound).astype(held_as)


def setup_inputs(seed: int = 0) -> dict:
    splits = jax.random.split(jax.random.key(seed), 9)
    features_t = noise(splits[0], (F_IN, VERTICES), 4.0, 24.0, ((0, 4), (1, 64)))
    weight = noise(splits[1], (F_IN, F_OUT), (F_IN // 4) ** -0.5, 1.0, ((0, 4),))
    bias = noise(splits[2], (F_OUT,), 0.5, 3.0, ((0, 4),), jnp.float32)
    self_mask = with_ends((jax.random.randint(splits[3], (N_VERT, BLOCK, BLOCK), 0, BLOCK) < 16).astype(jnp.int32), jax.random.fold_in(splits[3], 1), 0, 1)
    halo_mask = with_ends((jax.random.randint(splits[4], (N_VERT, NB, BLOCK, HALO), 0, HALO) < 8).astype(jnp.int32), jax.random.fold_in(splits[4], 1), 0, 1)
    block_src = draw_block_src(jax.random.fold_in(splits[8], 71), 0)
    halo_rows = draw_halo_rows(jax.random.fold_in(splits[8], 71), 0)
    outside_degree = with_ends(jax.random.randint(splits[7], (VERTICES,), 0, 48), jax.random.fold_in(splits[7], 1), 0, 47).astype(jnp.int32)
    return dict(features_t=features_t, weight=weight, bias=bias, self_mask=self_mask, halo_mask=halo_mask, block_src=block_src, halo_rows=halo_rows, outside_degree=outside_degree)


def reference(features_t, weight, bias, self_mask, halo_mask, block_src, halo_rows, outside_degree):
    live_slot = block_src >= 0
    halo_counts = lax.optimization_barrier(jnp.sum(lax.optimization_barrier(jnp.sum(halo_mask, axis=-1)) * live_slot[:, :, None].astype(jnp.int32), axis=1))
    degree = 1 + lax.optimization_barrier(jnp.sum(self_mask, axis=-1)) + halo_counts + outside_degree.reshape(N_VERT, BLOCK)
    inverse_root = 1.0 / jnp.sqrt(degree.astype(jnp.float32))
    flat_root = inverse_root.reshape(-1)
    scaled = (features_t.astype(jnp.float32) * flat_root[None, :]).astype(jnp.bfloat16)
    scaled_wide = scaled.astype(jnp.float32)

    def one_partition(inputs):
        part_index, own_mask, slot_masks, sources, rows, root_part = inputs
        own_block = lax.dynamic_slice_in_dim(scaled_wide, (part_index * BLOCK).astype(jnp.int32), BLOCK, 1)
        summed_rows = own_block + jnp.einsum('fj,ij->fi', own_block, own_mask.astype(jnp.float32))
        column_ids = (jnp.maximum(sources, 0) * BLOCK)[:, None] + rows
        halo_vals = jnp.take(scaled_wide, column_ids.reshape(-1).astype(jnp.int32), axis=1).reshape(F_IN, NB, HALO)
        live_blocks = slot_masks.astype(jnp.float32) * (sources >= 0).astype(jnp.float32)[:, None, None]
        summed_rows = summed_rows + jnp.einsum('fsk,sik->fi', halo_vals, live_blocks)
        return (summed_rows * root_part[None, :]).astype(jnp.bfloat16)
    parts_out = lax.map(one_partition, (jnp.arange(N_VERT, dtype=jnp.int32), self_mask, halo_mask, block_src, halo_rows, inverse_root))
    aggregated = jnp.transpose(parts_out, (1, 0, 2)).reshape(F_IN, N_VERT * BLOCK)
    mixed = jnp.dot(weight.T, aggregated, preferred_element_type=jnp.float32)
    return jnp.maximum(mixed + bias[:, None], 0.0).astype(jnp.bfloat16)
```

```python
import jax
import jax.numpy as jnp
from jax import lax
from jax.experimental import pallas as pl
from jax.experimental.pallas import tpu as pltpu
from jax.sharding import Mesh
from jax.sharding import PartitionSpec as P

VERT = ("x", "z", "core")
OFFSETS = (0, -3, 3, -1, -4, 2, 1, -2)
LANES = 128


def shifted(array, axis, by):
    count = lax.axis_size(axis)
    return lax.ppermute(array, axis, [(i, (i + by) % count) for i in range(count)])


def select_kernel(table, *refs):
    requests, pieces, outs, held = refs[:4], refs[4:10], refs[10:14], refs[14]
    first = 0
    for piece in pieces:
        for k in range(piece.shape[0] // 32):
            held[first] = piece[k * 32 : (k + 1) * 32, :].astype(jnp.float32)
            first += 1
    for k in range(4):
        outs[k][...] = jnp.zeros_like(outs[k])
        for s in range(6):
            which = table[k * 6 + s]

            @pl.when(which >= 0)
            def _():
                for g in range(2):
                    rows = requests[k][s : s + 1, g * LANES : (g + 1) * LANES]
                    rows = jnp.broadcast_to(rows, (32, LANES))
                    lane = rows & (LANES - 1)
                    block = rows >> 7
                    picked = jnp.zeros((32, LANES), jnp.float32)
                    for t in range(4):
                        part = held[which, :, t * LANES : (t + 1) * LANES]
                        took = jnp.take_along_axis(part, lane, axis=1, mode="promise_in_bounds")
                        picked = jnp.where(block == t, took, picked)
                    at = s * 256 + g * LANES
                    outs[k][:, at : at + LANES] = picked.astype(jnp.bfloat16)


def selected(table, requests, pieces):
    vmem = pl.BlockSpec(memory_space=pltpu.VMEM)
    return pl.pallas_call(
        select_kernel,
        out_shape=[jax.ShapeDtypeStruct((32, 1536), jnp.bfloat16)] * 4,
        in_specs=[pl.BlockSpec(memory_space=pltpu.SMEM)] + [vmem] * 10,
        out_specs=[vmem] * 4,
        scratch_shapes=[pltpu.VMEM((16, 32, 512), jnp.float32)],
        compiler_params=pltpu.CompilerParams(vmem_limit_bytes=8 * 2**20),
        name="select",
    )(table, *requests, *pieces)


def body(features_t, weight, bias, self_mask, halo_mask, block_src, halo_rows, outside_degree):
    sources = block_src[0]
    rows = halo_rows[0]
    my_x, my_z, my_core = (lax.axis_index(a) for a in VERT)
    live_slot = sources >= 0
    live_blocks = halo_mask[0] * live_slot.astype(jnp.int32)[:, None, None]
    degree = (
        1
        + jnp.sum(self_mask[0], axis=-1)
        + jnp.sum(jnp.sum(live_blocks, axis=-1), axis=0)
        + outside_degree
    )
    inverse_root = 1.0 / jnp.sqrt(degree.astype(jnp.float32))
    scaled = (features_t.astype(jnp.float32) * inverse_root[None, :]).astype(jnp.bfloat16)

    low = shifted(scaled, "z", 3)
    high = shifted(scaled, "z", -3)
    first = jnp.concatenate([scaled, low, high], axis=0)
    after = shifted(first, "z", 1)
    before = shifted(first[:64], "z", -1)

    request = jnp.concatenate(
        [rows, jnp.broadcast_to(jnp.pad(sources, (0, 250), constant_values=-1)[None], (2, 256))], axis=0
    )
    requests = [request] + [shifted(request, "x", -k) for k in (1, 2, 3)]
    wanted = jnp.stack([r[6, :6] for r in requests])
    apart = (wanted >> 1) - my_z
    place = jnp.zeros_like(wanted)
    for at, offset in enumerate(OFFSETS):
        place = jnp.where((apart & 7) == offset % 8, at, place)
    place = place + jnp.where((wanted & 1) == my_core, 0, 8)
    here = (wanted >= 0) & ((wanted >> 4) == my_x)
    table = jnp.where(here, place, -1).reshape(-1)

    own = (first, after, before)
    other = tuple(shifted(p, "core", 1) for p in own)
    picked = selected(table, requests, own + other)
    halo_vals = picked[0]
    for k in (1, 2, 3):
        halo_vals = halo_vals + shifted(picked[k], "x", k)
    halo_vals = halo_vals.reshape(32, 6, 256)

    summed_rows = scaled.astype(jnp.float32) + lax.dot_general(
        scaled, self_mask[0].astype(jnp.bfloat16), (((1,), (1,)), ((), ())), preferred_element_type=jnp.float32
    )
    summed_rows = summed_rows + jnp.einsum(
        "fsk,sik->fi", halo_vals, halo_mask[0].astype(jnp.bfloat16), preferred_element_type=jnp.float32
    )
    aggregated = (summed_rows * inverse_root[None, :]).astype(jnp.bfloat16)

    my_af = lax.axis_index("af")

    def columns(of):
        return lax.dynamic_slice_in_dim(weight, of * 64, 64, 1)

    mixed = None
    for k in range(4):
        weight_k = columns(jnp.mod(my_af + k, 4))
        inputs_k = aggregated
        if k:
            weight_k = shifted(weight_k, "af", k)
            inputs_k = shifted(aggregated, "af", k)
        term = lax.dot_general(
            weight_k, inputs_k, (((0,), (0,)), ((), ())), preferred_element_type=jnp.float32
        )
        mixed = term if mixed is None else mixed + term
    return jnp.maximum(mixed + bias[:, None], 0.0).astype(jnp.bfloat16)


def solution(mesh):
    finer = Mesh(mesh.devices.reshape(4, 8, 2, 4), ("x", "z", "core", "af"))
    return jax.shard_map(
        body,
        mesh=finer,
        in_specs=(
            P("af", VERT),
            P("af", None),
            P("af"),
            P(VERT, None, None),
            P(VERT, None, None, None),
            P(VERT, None),
            P(VERT, None, None),
            P(VERT),
        ),
        out_specs=P("af", VERT),
        check_vma=False,
    )
```

```python
import jax
import jax.numpy as jnp
from jax import lax
from jax.experimental import pallas as pl
from jax.experimental.pallas import tpu as pltpu
from jax.sharding import Mesh
from jax.sharding import PartitionSpec as P


VERT = ("x", "z", "core")
LANES = 128
FEATS = 32
VMEM = pltpu.VMEM
CHUNKS = 4
ROWS = 512 // CHUNKS


def shifted(array, axis, by):
    count = lax.axis_size(axis)
    return lax.ppermute(array, axis, [(i, (i + by) % count) for i in range(count)])


def opposed(array, by):
    count = lax.axis_size("z")
    pairs = [(2 * z + c, 2 * ((z + (by, -by)[c]) % count) + c) for z in range(count) for c in range(2)]
    return lax.ppermute(array, ("z", "core"), pairs)


def whole(count=1):
    return [pl.BlockSpec(memory_space=VMEM)] * count


def in_hbm(array):
    return pltpu.with_memory_space_constraint(array, pltpu.HBM)


def head_kernel(
    sources_in, self_in, halo_in, outside_in, features_in, rows_in,
    scaled, root, request,
    sources, self_mask, halo_mask, outside, features, rows, small, large,
):
    smalls = [
        pltpu.make_async_copy(src, dst, small.at[k])
        for k, (src, dst) in enumerate(
            (
                (sources_in, sources),
                (outside_in, outside),
                (features_in, features),
                (rows_in, rows),
            )
        )
    ]
    larges = []
    for r in range(CHUNKS):
        at = pl.ds(r * ROWS, ROWS)
        larges.append(pltpu.make_async_copy(halo_in.at[0, :, at, :], halo_mask.at[:, at, :], large.at[r, 0]))
        larges.append(pltpu.make_async_copy(self_in.at[0, at, :], self_mask.at[at, :], large.at[r, 1]))
    smalls[0].start()
    for copy in larges[:2] + smalls[1:] + larges[2:]:
        copy.start()
    for copy in smalls:
        copy.wait()

    for s in range(6):
        for g in range(2):
            request[s : s + 1, g * LANES : (g + 1) * LANES] = rows[2 * s + g]
    lane = lax.broadcasted_iota(jnp.int32, (2, 256), 1)
    listed = jnp.full((2, 256), -1, jnp.int32)
    for s in range(6):
        listed = jnp.where(lane == s, sources[0, s], listed)
    request[6:8, :] = listed

    ones = jnp.ones((8, LANES), jnp.bfloat16)
    live = [(sources[0, s] >= 0).astype(jnp.int32) for s in range(6)]
    for r in range(CHUNKS):
        larges[2 * r].wait()
        larges[2 * r + 1].wait()
        at = slice(r * ROWS, (r + 1) * ROWS)
        total = self_mask[at, :LANES]
        for t in range(1, 4):
            total = total + self_mask[at, t * LANES : (t + 1) * LANES]
        for s in range(6):
            total = total + (halo_mask[s, at, :LANES] + halo_mask[s, at, LANES:]) * live[s]
        counts = total.astype(jnp.float32).astype(jnp.bfloat16)
        summed = lax.dot_general(ones, counts, (((1,), (1,)), ((), ())), preferred_element_type=jnp.float32)
        degree = summed[:1] + 1.0 + outside[:, at].astype(jnp.float32)
        inverse = 1.0 / jnp.sqrt(degree)
        root[:, at] = inverse
        scaled[:, at] = (features[:, at].astype(jnp.float32) * inverse).astype(jnp.bfloat16)


def head(block_src, self_mask, halo_mask, outside_degree, features_t, halo_rows):
    return pl.pallas_call(
        head_kernel,
        out_shape=[
            pltpu.VMEM((FEATS, 512), jnp.bfloat16),
            pltpu.VMEM((1, 512), jnp.float32),
            pltpu.VMEM((8, 256), jnp.int32),
        ],
        in_specs=[pl.BlockSpec(memory_space=pltpu.HBM)] * 6,
        out_specs=whole(3),
        scratch_shapes=[
            pltpu.SMEM((1, 6), jnp.int32),
            VMEM((512, 512), jnp.int32),
            VMEM((6, 512, 256), jnp.int32),
            VMEM((1, 512), jnp.int32),
            VMEM((FEATS, 512), jnp.bfloat16),
            VMEM((12, 1, LANES), jnp.int32),
            pltpu.SemaphoreType.DMA((4,)),
            pltpu.SemaphoreType.DMA((CHUNKS, 2)),
        ],
        compiler_params=pltpu.CompilerParams(vmem_limit_bytes=8 * 2**20),
        name="head",
    )(
        *map(
            in_hbm,
            (
                block_src,
                self_mask,
                halo_mask,
                outside_degree.reshape(1, 512),
                features_t,
                halo_rows.reshape(12, 1, LANES),
            ),
        )
    )


def select_kernel(table, *refs):
    requests, pieces, outs, held = refs[:4], refs[4:-5], refs[-5:-1], refs[-1]
    first = 0
    for piece in pieces:
        for k in range(piece.shape[0] // FEATS):
            held[first] = piece[k * FEATS : (k + 1) * FEATS, :].astype(jnp.float32)
            first += 1
    for k in range(4):
        outs[k][...] = jnp.zeros_like(outs[k])
        for s in range(6):
            which = table[k * 256 + s]

            @pl.when(which >= 0)
            def _():
                for g in range(2):
                    rows = requests[k][s : s + 1, g * LANES : (g + 1) * LANES]
                    rows = jnp.broadcast_to(rows, (FEATS, LANES))
                    lane = rows & (LANES - 1)
                    block = rows >> 7
                    picked = jnp.zeros((FEATS, LANES), jnp.float32)
                    for t in range(4):
                        part = held[which, :, t * LANES : (t + 1) * LANES]
                        took = jnp.take_along_axis(part, lane, axis=1, mode="promise_in_bounds")
                        picked = jnp.where(block == t, took, picked)
                    at = s * 256 + g * LANES
                    outs[k][:, at : at + LANES] = picked.astype(jnp.bfloat16)


def selected(table, requests, pieces):
    return pl.pallas_call(
        select_kernel,
        out_shape=[pltpu.VMEM((FEATS, 1536), jnp.bfloat16)] * 4,
        in_specs=[pl.BlockSpec(memory_space=pltpu.SMEM)] + whole(4 + len(pieces)),
        out_specs=whole(4),
        scratch_shapes=[pltpu.VMEM((16, FEATS, 512), jnp.float32)],
        compiler_params=pltpu.CompilerParams(vmem_limit_bytes=8 * 2**20),
        name="select",
    )(table, *requests, *pieces)


def prepare_kernel(halo_mask, turned):
    turned[...] = halo_mask[0, 0].astype(jnp.float32).T.astype(jnp.bfloat16)


def prepared(halo_mask):
    return pl.pallas_call(
        prepare_kernel,
        grid=(6,),
        out_shape=pltpu.VMEM((1536, 512), jnp.bfloat16),
        in_specs=[pl.BlockSpec((1, 1, 512, 256), lambda s: (0, s, 0, 0))],
        out_specs=pl.BlockSpec((256, 512), lambda s: (s, 0)),
        compiler_params=pltpu.CompilerParams(vmem_limit_bytes=8 * 2**20),
        name="prepare",
    )(in_hbm(halo_mask))


def aggregate_kernel(mine, one, two, three, turned, begun, root, columns, *outs):
    halo_vals = mine[...] + one[...] + two[...] + three[...]
    summed = begun[...] + jnp.dot(halo_vals, turned[...], preferred_element_type=jnp.float32)
    aggregated = (summed * root[...]).astype(jnp.bfloat16)
    for k in range(4):
        outs[k][:, :512] = aggregated
        outs[k][:, 512:] = columns[k]


def aggregate(vals, turned, begun, root, columns):
    return pl.pallas_call(
        aggregate_kernel,
        out_shape=[pltpu.VMEM((FEATS, 640), jnp.bfloat16)] * 4,
        in_specs=whole(8),
        out_specs=whole(4),
        compiler_params=pltpu.CompilerParams(vmem_limit_bytes=8 * 2**20),
        name="aggregate",
    )(*vals, turned, begun, root, columns)


def mix_kernel(*refs):
    parts, bias, out = refs[:4], refs[4], refs[5]
    mixed = jnp.broadcast_to(bias[...], (64, 512))
    for part in parts:
        mixed = mixed + lax.dot_general(
            part[:, 512 : 512 + 64], part[:, :512], (((0,), (0,)), ((), ())), preferred_element_type=jnp.float32
        )
    out[...] = jnp.maximum(mixed, 0.0).astype(jnp.bfloat16)


def mix(parts, bias):
    return pl.pallas_call(
        mix_kernel,
        out_shape=jax.ShapeDtypeStruct((64, 512), jnp.bfloat16),
        in_specs=whole(5),
        out_specs=whole(1)[0],
        compiler_params=pltpu.CompilerParams(vmem_limit_bytes=8 * 2**20),
        name="mix",
    )(*parts, bias.reshape(64, 1))


def piece_table(requests):
    my_x, my_z, my_core = (lax.axis_index(a) for a in VERT)
    wanted = jnp.concatenate([r[6] for r in requests])
    ahead = (wanted >> 1) - my_z
    ahead = jnp.where(my_core == 0, -ahead, ahead) & 7
    same = (wanted & 1) == my_core
    place = jnp.zeros_like(wanted)
    for distance, (ours, theirs) in enumerate(
        ((0, 1), (4, 5), (2, 3), (6, 7), (8, 15), (14, 13), (10, 9), (12, 11))
    ):
        place = jnp.where(ahead == distance, jnp.where(same, ours, theirs), place)
    here = (wanted >= 0) & ((wanted >> 4) == my_x)
    return jnp.where(here, place, -1)


def body(features_t, weight, bias, self_mask, halo_mask, block_src, halo_rows, outside_degree):
    scaled, root, request = head(block_src, self_mask, halo_mask, outside_degree, features_t, halo_rows)

    partner = shifted(scaled, "core", 1)
    both = jnp.concatenate([scaled, partner], axis=0)
    two = opposed(both, 2)
    four = shifted(scaled, "z", 4)
    one = opposed(jnp.concatenate([both, two], axis=0), 1)
    requests = [request]
    for k in (1, 2, 3):
        requests.append(shifted(request, "x", -k))
    table = piece_table(requests)
    rest = []
    for piece in (two, one, four):
        rest.append(shifted(piece, "core", 1))
    picked = selected(table, requests, (scaled, partner, two, one, four, *rest))
    vals = [picked[0]]
    for k in (1, 2, 3):
        vals.append(shifted(picked[k], "x", k))

    late_halo, late_self, _ = lax.optimization_barrier((halo_mask, self_mask, picked[0]))
    turned = prepared(late_halo)
    begun = scaled.astype(jnp.float32) + lax.dot_general(
        scaled, late_self[0].astype(jnp.bfloat16), (((1,), (1,)), ((), ())), preferred_element_type=jnp.float32
    )
    my_af = lax.axis_index("af")
    columns = jnp.stack(
        [
            jnp.pad(lax.dynamic_slice_in_dim(weight, jnp.mod(my_af + k, 4) * 64, 64, 1), ((0, 0), (0, 64)))
            for k in range(4)
        ]
    )
    sent = aggregate(vals, turned, begun, root, columns)
    parts = [sent[0]]
    for k in (1, 2, 3):
        parts.append(shifted(sent[k], "af", k))
    return mix(parts, bias)


def solution(mesh):
    finer = Mesh(mesh.devices.reshape(4, 8, 2, 4), ("x", "z", "core", "af"))
    return jax.shard_map(
        body,
        mesh=finer,
        in_specs=(
            P("af", VERT),
            P("af", None),
            P("af"),
            P(VERT, None, None),
            P(VERT, None, None, None),
            P(VERT, None),
            P(VERT, None, None),
            P(VERT),
        ),
        out_specs=P("af", VERT),
        check_vma=False,
    )
```

```python
import jax
import jax.numpy as jnp
from jax import lax
from jax.experimental import pallas as pl
from jax.experimental.pallas import tpu as pltpu
from jax.sharding import Mesh
from jax.sharding import PartitionSpec as P


VERT = ("x", "z", "core")
LANES = 128
FEATS = 32
SURE = 3
VMEM = pltpu.VMEM


def shifted(array, axis, by):
    count = lax.axis_size(axis)
    return lax.ppermute(array, axis, [(i, (i + by) % count) for i in range(count)])


def paired(array, axis, by):
    return lax.ppermute(array, axis, [(i, i ^ by) for i in range(lax.axis_size(axis))])


def opposed(array, by):
    count = lax.axis_size("z")
    pairs = [(2 * z + c, 2 * ((z + (by, -by)[c]) % count) + c) for z in range(count) for c in range(2)]
    return lax.ppermute(array, ("z", "core"), pairs)


def whole(count=1):
    return [pl.BlockSpec(memory_space=VMEM)] * count


def in_hbm(array):
    return pltpu.with_memory_space_constraint(array, pltpu.HBM)


def head_kernel(
    sources_in, self_in, halo_in, outside_in, features_in, rows_in,
    scaled, root, request, self_out, halo_out,
    sources, self_mask, halo_mask, outside, features, rows, total, small, own, slot,
):
    smalls = [
        pltpu.make_async_copy(src, dst, small.at[k])
        for k, (src, dst) in enumerate(
            (
                (sources_in, sources),
                (outside_in, outside),
                (features_in, features),
                (rows_in, rows),
            )
        )
    ]
    owns = [
        pltpu.make_async_copy(
            self_in.at[0, pl.ds(r * 256, 256), :], self_mask.at[pl.ds(r * 256, 256), :], own.at[r]
        )
        for r in range(2)
    ]
    slots = [pltpu.make_async_copy(halo_in.at[0, s], halo_mask.at[s], slot.at[s]) for s in range(6)]
    smalls[0].start()
    owns[0].start()
    owns[1].start()
    for s in range(SURE):
        slots[s].start()
    for copy in smalls[1:]:
        copy.start()
    smalls[0].wait()
    for s in range(SURE, 6):
        pl.when(sources[0, s] >= 0)(slots[s].start)
    for copy in smalls[1:]:
        copy.wait()

    for s in range(6):
        for g in range(2):
            request[s : s + 1, g * LANES : (g + 1) * LANES] = rows[2 * s + g]
    lane = lax.broadcasted_iota(jnp.int32, (2, 256), 1)
    listed = jnp.full((2, 256), -1, jnp.int32)
    for s in range(6):
        listed = jnp.where(lane == s, sources[0, s], listed)
    request[6:8, :] = listed

    for r in range(2):
        owns[r].wait()
        at = slice(r * 256, (r + 1) * 256)
        block = self_mask[at, :]
        self_out[at, :] = block.astype(jnp.float32).astype(jnp.bfloat16)
        total[at, :] = (block[:, :128] + block[:, 128:256]) + (block[:, 256:384] + block[:, 384:])
    for s in range(6):

        if s < SURE:
            slots[s].wait()

        def counted(s=s):
            if s >= SURE:
                slots[s].wait()
            block = halo_mask[s]
            halo_out[s] = block.astype(jnp.float32).astype(jnp.bfloat16)
            total[...] += block[:, :LANES] + block[:, LANES:]

        def left_out(s=s):
            halo_out[s] = jnp.zeros_like(halo_out[s])

        if s:
            live = sources[0, s] >= 0
            pl.when(live)(counted)
            pl.when(jnp.logical_not(live))(left_out)
        else:
            counted()
    ones = jnp.ones((8, LANES), jnp.bfloat16)
    counts = total[...].astype(jnp.float32).astype(jnp.bfloat16)
    summed = lax.dot_general(ones, counts, (((1,), (1,)), ((), ())), preferred_element_type=jnp.float32)
    inverse = lax.rsqrt(summed[:1] + 1.0 + outside[...].astype(jnp.float32))
    root[...] = inverse
    scaled[...] = (features[...].astype(jnp.float32) * inverse).astype(jnp.bfloat16)


def head(block_src, self_mask, halo_mask, outside_degree, features_t, halo_rows):
    return pl.pallas_call(
        head_kernel,
        out_shape=[
            VMEM((FEATS, 512), jnp.bfloat16),
            VMEM((1, 512), jnp.float32),
            VMEM((8, 256), jnp.int32),
            VMEM((512, 512), jnp.bfloat16),
            VMEM((6, 512, 256), jnp.bfloat16),
        ],
        in_specs=[pl.BlockSpec(memory_space=pltpu.HBM)] * 6,
        out_specs=whole(5),
        scratch_shapes=[
            pltpu.SMEM((1, 6), jnp.int32),
            VMEM((512, 512), jnp.int32),
            VMEM((6, 512, 256), jnp.int32),
            VMEM((1, 512), jnp.int32),
            VMEM((FEATS, 512), jnp.bfloat16),
            VMEM((12, 1, LANES), jnp.int32),
            VMEM((512, LANES), jnp.int32),
            pltpu.SemaphoreType.DMA((4,)),
            pltpu.SemaphoreType.DMA((2,)),
            pltpu.SemaphoreType.DMA((6,)),
        ],
        compiler_params=pltpu.CompilerParams(vmem_limit_bytes=8 * 2**20),
        name="head",
    )(
        *map(
            in_hbm,
            (
                block_src,
                self_mask,
                halo_mask,
                outside_degree.reshape(1, 512),
                features_t,
                halo_rows.reshape(12, 1, LANES),
            ),
        )
    )


def select_kernel(listed, *refs):
    requests, pieces, outs, (held, table, arrived) = refs[:4], refs[4:-7], refs[-7:-3], refs[-3:]
    tables = pltpu.make_async_copy(listed, table, arrived)
    tables.start()
    at = 0
    for piece in pieces:
        for k in range(piece.shape[0] // FEATS):
            held[at] = piece[k * FEATS : (k + 1) * FEATS, :].astype(jnp.float32)
            at += 1
    for out in outs:
        out[...] = jnp.zeros_like(out)
    tables.wait()
    for k in range(4):
        for s in range(6):
            which = table[k, s]

            @pl.when(which >= 0)
            def _():
                for g in range(2):
                    rows = requests[k][s : s + 1, g * LANES : (g + 1) * LANES]
                    rows = jnp.broadcast_to(rows, (FEATS, LANES))
                    lane = rows & (LANES - 1)
                    block = rows >> 7
                    picked = jnp.zeros((FEATS, LANES), jnp.float32)
                    for t in range(4):
                        part = held[which, :, t * LANES : (t + 1) * LANES]
                        took = jnp.take_along_axis(part, lane, axis=1, mode="promise_in_bounds")
                        picked = jnp.where(block == t, took, picked)
                    to = s * 256 + g * LANES
                    outs[k][:, to : to + LANES] = picked.astype(jnp.bfloat16)


def selected(table, requests, pieces):
    operands = (table, *requests, *pieces)
    return pl.pallas_call(
        select_kernel,
        out_shape=[VMEM((FEATS, 1536), jnp.bfloat16)] * 4,
        in_specs=whole(len(operands)),
        out_specs=whole(4),
        scratch_shapes=[
            VMEM((16, FEATS, 512), jnp.float32),
            pltpu.SMEM((4, LANES), jnp.int32),
            pltpu.SemaphoreType.DMA,
        ],
        compiler_params=pltpu.CompilerParams(vmem_limit_bytes=8 * 2**20),
        name="select",
    )(*operands)


def join_kernel(*refs):
    at = 0
    for piece in refs[:-1]:
        refs[-1][at : at + piece.shape[0], :] = piece[...]
        at += piece.shape[0]


def joined(*pieces):
    return pl.pallas_call(
        join_kernel,
        out_shape=VMEM((sum(p.shape[0] for p in pieces), 512), jnp.bfloat16),
        in_specs=whole(len(pieces)),
        out_specs=whole()[0],
        compiler_params=pltpu.CompilerParams(vmem_limit_bytes=2 * 2**20),
        name="join",
    )(*pieces)


def prepare_kernel(halo_mask, self_mask, scaled, turned, begun):
    for s in range(6):
        turned[s * 256 : (s + 1) * 256, :] = halo_mask[s].T
    begun[...] = scaled[...].astype(jnp.float32) + lax.dot_general(
        scaled[...], self_mask[...], (((1,), (1,)), ((), ())), preferred_element_type=jnp.float32
    )


def prepared(halo_mask, self_mask, scaled):
    return pl.pallas_call(
        prepare_kernel,
        out_shape=[VMEM((1536, 512), jnp.bfloat16), VMEM((FEATS, 512), jnp.float32)],
        in_specs=whole(3),
        out_specs=whole(2),
        compiler_params=pltpu.CompilerParams(vmem_limit_bytes=16 * 2**20),
        name="prepare",
    )(halo_mask, self_mask, scaled)


def aggregate_kernel(mine, one, two, three, turned, begun, root, columns, *outs):
    halo_vals = mine[...] + one[...] + two[...] + three[...]
    summed = begun[...] + jnp.dot(halo_vals, turned[...], preferred_element_type=jnp.float32)
    aggregated = (summed * root[...]).astype(jnp.bfloat16)
    for k in range(4):
        outs[k][:, :512] = aggregated
        outs[k][:, 512:] = columns[k]


def aggregate(vals, turned, begun, root, columns):
    return pl.pallas_call(
        aggregate_kernel,
        out_shape=[VMEM((FEATS, 640), jnp.bfloat16)] * 4,
        in_specs=whole(8),
        out_specs=whole(4),
        compiler_params=pltpu.CompilerParams(vmem_limit_bytes=8 * 2**20),
        name="aggregate",
    )(*vals, turned, begun, root, columns)


def mix_kernel(*refs):
    parts, bias, out = refs[:4], refs[4], refs[5]
    mixed = jnp.broadcast_to(bias[...], (64, 512))
    for part in parts:
        mixed = mixed + lax.dot_general(
            part[:, 512 : 512 + 64], part[:, :512], (((0,), (0,)), ((), ())), preferred_element_type=jnp.float32
        )
    out[...] = jnp.maximum(mixed, 0.0).astype(jnp.bfloat16)


def mix(parts, bias):
    return pl.pallas_call(
        mix_kernel,
        out_shape=jax.ShapeDtypeStruct((64, 512), jnp.bfloat16),
        in_specs=whole(5),
        out_specs=whole(1)[0],
        compiler_params=pltpu.CompilerParams(vmem_limit_bytes=8 * 2**20),
        name="mix",
    )(*parts, bias.reshape(64, 1))


def piece_table(requests):
    my_x, my_z, my_core = (lax.axis_index(a) for a in VERT)
    wanted = jnp.concatenate([r[6:7, :LANES] for r in requests], axis=0)
    ahead = (wanted >> 1) - my_z
    ahead = jnp.where(my_core == 0, -ahead, ahead) & 7
    same = (wanted & 1) == my_core
    place = jnp.zeros_like(wanted)
    for distance, (ours, theirs) in enumerate(
        ((0, 1), (4, 5), (2, 3), (6, 7), (8, 15), (14, 13), (10, 9), (12, 11))
    ):
        place = jnp.where(ahead == distance, jnp.where(same, ours, theirs), place)
    here = (wanted >= 0) & ((wanted >> 4) == my_x)
    return jnp.where(here, place, -1)


def body(features_t, weight, bias, self_mask, halo_mask, block_src, halo_rows, outside_degree):
    scaled, root, request, held_self, held_halo = head(block_src, self_mask, halo_mask, outside_degree, features_t, halo_rows)

    partner = shifted(scaled, "core", 1)
    both = joined(scaled, partner)
    two = opposed(both, 2)
    turned, begun = prepared(held_halo, held_self, scaled)
    weight, bias, _ = lax.optimization_barrier((weight, bias, begun))
    four = shifted(scaled, "z", 4)
    one = opposed(joined(both, two), 1)
    requests = [request]
    for k in (1, 2, 3):
        requests.append(paired(request, "x", k))
    *requests, _ = lax.optimization_barrier((*requests, begun))
    table = piece_table(requests)
    rest = []
    for piece in (two, one, four):
        rest.append(shifted(piece, "core", 1))
    picked = selected(table, requests, (scaled, partner, two, one, four, *rest))
    vals = [picked[0]]
    for k in (1, 2, 3):
        vals.append(paired(picked[k], "x", k))

    my_af = lax.axis_index("af")
    columns = jnp.stack(
        [
            jnp.pad(lax.dynamic_slice_in_dim(weight, (my_af ^ k) * 64, 64, 1), ((0, 0), (0, 64)))
            for k in range(4)
        ]
    )
    sent = aggregate(vals, turned, begun, root, columns)
    parts = [sent[0]]
    for k in (1, 2, 3):
        parts.append(paired(sent[k], "af", k))
    return mix(parts, bias)


def solution(mesh):
    finer = Mesh(mesh.devices.reshape(4, 8, 2, 4), ("x", "z", "core", "af"))
    return jax.shard_map(
        body,
        mesh=finer,
        in_specs=(
            P("af", VERT),
            P("af", None),
            P("af"),
            P(VERT, None, None),
            P(VERT, None, None, None),
            P(VERT, None),
            P(VERT, None, None),
            P(VERT),
        ),
        out_specs=P("af", VERT),
        check_vma=False,
    )
```

```python
import functools

import jax
import jax.numpy as jnp
from jax import lax
from jax.experimental import pallas as pl
from jax.experimental.pallas import tpu as pltpu
from jax.sharding import Mesh
from jax.sharding import PartitionSpec as P


VERT = ("x", "z", "core")
LANES = 128
FEATS = 32
SURE = 3
VMEM = pltpu.VMEM


def shifted(array, axis, by):
    count = lax.axis_size(axis)
    return lax.ppermute(array, axis, [(i, (i + by) % count) for i in range(count)])


def paired(array, axis, by):
    return lax.ppermute(array, axis, [(i, i ^ by) for i in range(lax.axis_size(axis))])


def opposed(array, by):
    count = lax.axis_size("z")
    pairs = [(2 * z + c, 2 * ((z + (by, -by)[c]) % count) + c) for z in range(count) for c in range(2)]
    return lax.ppermute(array, ("z", "core"), pairs)


def whole(count=1):
    return [pl.BlockSpec(memory_space=VMEM)] * count


def in_hbm(array):
    return pltpu.with_memory_space_constraint(array, pltpu.HBM)


def head_kernel(
    sources_in, self_in, halo_in, outside_in, features_in, rows_in,
    scaled, root, request, self_out, halo_out,
    sources, self_mask, halo_mask, outside, features, rows, total, small, own, slot,
):
    smalls = [
        pltpu.make_async_copy(src, dst, small.at[k])
        for k, (src, dst) in enumerate(
            (
                (sources_in, sources),
                (outside_in, outside),
                (features_in, features),
                (rows_in, rows),
            )
        )
    ]
    owns = [
        pltpu.make_async_copy(
            self_in.at[0, pl.ds(r * 256, 256), :], self_mask.at[pl.ds(r * 256, 256), :], own.at[r]
        )
        for r in range(2)
    ]
    slots = [pltpu.make_async_copy(halo_in.at[0, s], halo_mask.at[s], slot.at[s]) for s in range(6)]
    smalls[0].start()
    owns[0].start()
    owns[1].start()
    for s in range(SURE):
        slots[s].start()
    for copy in smalls[1:]:
        copy.start()
    smalls[0].wait()
    for s in range(SURE, 6):
        pl.when(sources[0, s] >= 0)(slots[s].start)
    for copy in smalls[1:]:
        copy.wait()

    for s in range(6):
        for g in range(2):
            request[s : s + 1, g * LANES : (g + 1) * LANES] = rows[2 * s + g]
    lane = lax.broadcasted_iota(jnp.int32, (2, 256), 1)
    listed = jnp.full((2, 256), -1, jnp.int32)
    for s in range(6):
        listed = jnp.where(lane == s, sources[0, s], listed)
    request[6:8, :] = listed

    for r in range(2):
        owns[r].wait()
        at = slice(r * 256, (r + 1) * 256)
        block = self_mask[at, :]
        self_out[at, :] = block.astype(jnp.float32).astype(jnp.bfloat16)
        total[at, :] = (block[:, :128] + block[:, 128:256]) + (block[:, 256:384] + block[:, 384:])
    for s in range(6):

        if s < SURE:
            slots[s].wait()

        def counted(s=s):
            if s >= SURE:
                slots[s].wait()
            block = halo_mask[s]
            halo_out[s] = block.astype(jnp.float32).astype(jnp.bfloat16)
            total[...] += block[:, :LANES] + block[:, LANES:]

        def left_out(s=s):
            halo_out[s] = jnp.zeros_like(halo_out[s])

        if s:
            live = sources[0, s] >= 0
            pl.when(live)(counted)
            pl.when(jnp.logical_not(live))(left_out)
        else:
            counted()
    ones = jnp.ones((8, LANES), jnp.bfloat16)
    counts = total[...].astype(jnp.float32).astype(jnp.bfloat16)
    summed = lax.dot_general(ones, counts, (((1,), (1,)), ((), ())), preferred_element_type=jnp.float32)
    inverse = lax.rsqrt(summed[:1] + 1.0 + outside[...].astype(jnp.float32))
    root[...] = inverse
    scaled[...] = (features[...].astype(jnp.float32) * inverse).astype(jnp.bfloat16)


def head(block_src, self_mask, halo_mask, outside_degree, features_t, halo_rows):
    return pl.pallas_call(
        head_kernel,
        out_shape=[
            VMEM((FEATS, 512), jnp.bfloat16),
            VMEM((1, 512), jnp.float32),
            VMEM((8, 256), jnp.int32),
            VMEM((512, 512), jnp.bfloat16),
            VMEM((6, 512, 256), jnp.bfloat16),
        ],
        in_specs=[pl.BlockSpec(memory_space=pltpu.HBM)] * 6,
        out_specs=whole(5),
        scratch_shapes=[
            pltpu.SMEM((1, 6), jnp.int32),
            VMEM((512, 512), jnp.int32),
            VMEM((6, 512, 256), jnp.int32),
            VMEM((1, 512), jnp.int32),
            VMEM((FEATS, 512), jnp.bfloat16),
            VMEM((12, 1, LANES), jnp.int32),
            VMEM((512, LANES), jnp.int32),
            pltpu.SemaphoreType.DMA((4,)),
            pltpu.SemaphoreType.DMA((2,)),
            pltpu.SemaphoreType.DMA((6,)),
        ],
        compiler_params=pltpu.CompilerParams(vmem_limit_bytes=8 * 2**20),
        name="head",
    )(
        *map(
            in_hbm,
            (
                block_src,
                self_mask,
                halo_mask,
                outside_degree.reshape(1, 512),
                features_t,
                halo_rows.reshape(12, 1, LANES),
            ),
        )
    )


def place_kernel(listed, table, arrived):
    copy = pltpu.make_async_copy(listed, table, arrived)
    copy.start()
    copy.wait()


def placed(listed):
    return pl.pallas_call(
        place_kernel,
        out_shape=pltpu.SMEM((4, LANES), jnp.int32),
        in_specs=whole(),
        out_specs=pl.BlockSpec(memory_space=pltpu.SMEM),
        scratch_shapes=[pltpu.SemaphoreType.DMA],
        compiler_params=pltpu.CompilerParams(vmem_limit_bytes=2**20),
        name="place",
    )(listed)


def select_kernel(dests, table, *refs):
    if dests == (0,):
        requests, refs = ((refs[0], 0),), refs[1:]
    else:
        requests, refs = ((refs[0], 0), (refs[1], 0), (refs[1], 8)), refs[2:]
    pieces, outs, held = refs[: -1 - len(dests)], refs[-1 - len(dests) : -1], refs[-1]
    at = 0
    for piece in pieces:
        for k in range(piece.shape[0] // FEATS):
            held[at] = piece[k * FEATS : (k + 1) * FEATS, :].astype(jnp.float32)
            at += 1
    for dest, (request, top), out in zip(dests, requests, outs):
        out[...] = jnp.zeros_like(out)
        for s in range(6):
            which = table[dest, s]

            @pl.when(which >= 0)
            def _():
                for g in range(2):
                    rows = request[top + s : top + s + 1, g * LANES : (g + 1) * LANES]
                    rows = jnp.broadcast_to(rows, (FEATS, LANES))
                    lane = rows & (LANES - 1)
                    block = rows >> 7
                    picked = jnp.zeros((FEATS, LANES), jnp.float32)
                    for t in range(4):
                        part = held[which, :, t * LANES : (t + 1) * LANES]
                        took = jnp.take_along_axis(part, lane, axis=1, mode="promise_in_bounds")
                        picked = jnp.where(block == t, took, picked)
                    to = s * 256 + g * LANES
                    out[:, to : to + LANES] = picked.astype(jnp.bfloat16)


def selected(dests, table, requests, pieces):
    operands = (*requests, *pieces)
    return pl.pallas_call(
        functools.partial(select_kernel, dests),
        out_shape=[VMEM((FEATS, 1536), jnp.bfloat16)] * len(dests),
        in_specs=[pl.BlockSpec(memory_space=pltpu.SMEM)] + whole(len(operands)),
        out_specs=whole(len(dests)),
        scratch_shapes=[VMEM((16, FEATS, 512), jnp.float32)],
        compiler_params=pltpu.CompilerParams(vmem_limit_bytes=8 * 2**20),
    )(pltpu.with_memory_space_constraint(table, pltpu.SMEM), *operands)


def join_kernel(*refs):
    at = 0
    for piece in refs[:-1]:
        refs[-1][at : at + piece.shape[0], :] = piece[...]
        at += piece.shape[0]


def joined(*pieces):
    return pl.pallas_call(
        join_kernel,
        out_shape=VMEM((sum(p.shape[0] for p in pieces), 512), jnp.bfloat16),
        in_specs=whole(len(pieces)),
        out_specs=whole()[0],
        compiler_params=pltpu.CompilerParams(vmem_limit_bytes=2 * 2**20),
        name="join",
    )(*pieces)


def prepare_kernel(halo_mask, self_mask, scaled, turned, begun):
    for s in range(6):
        turned[s * 256 : (s + 1) * 256, :] = halo_mask[s].T
    begun[...] = scaled[...].astype(jnp.float32) + lax.dot_general(
        scaled[...], self_mask[...], (((1,), (1,)), ((), ())), preferred_element_type=jnp.float32
    )


def prepared(halo_mask, self_mask, scaled):
    return pl.pallas_call(
        prepare_kernel,
        out_shape=[VMEM((1536, 512), jnp.bfloat16), VMEM((FEATS, 512), jnp.float32)],
        in_specs=whole(3),
        out_specs=whole(2),
        compiler_params=pltpu.CompilerParams(vmem_limit_bytes=16 * 2**20),
        name="prepare",
    )(halo_mask, self_mask, scaled)


def aggregate_kernel(mine, one, two, three, turned, begun, root, columns, *outs):
    halo_vals = mine[...] + one[...] + two[...] + three[...]
    summed = begun[...] + jnp.dot(halo_vals, turned[...], preferred_element_type=jnp.float32)
    aggregated = (summed * root[...]).astype(jnp.bfloat16)
    for k in range(4):
        outs[k][:, :512] = aggregated
        outs[k][:, 512:] = columns[k]


def aggregate(vals, turned, begun, root, columns):
    return pl.pallas_call(
        aggregate_kernel,
        out_shape=[VMEM((FEATS, 640), jnp.bfloat16)] * 4,
        in_specs=whole(8),
        out_specs=whole(4),
        compiler_params=pltpu.CompilerParams(vmem_limit_bytes=8 * 2**20),
        name="aggregate",
    )(*vals, turned, begun, root, columns)


def mixed(part):
    return lax.dot_general(
        part[:, 512:576], part[:, :512], (((0,), (0,)), ((), ())), preferred_element_type=jnp.float32
    )


def mix_kernel(bias, one, two, three, out):
    out[...] = bias[...] + mixed(one) + mixed(two) + mixed(three)


def finish_kernel(begun, part, out):
    out[...] = jnp.maximum(begun[...] + mixed(part), 0.0).astype(jnp.bfloat16)


def mix(bias, parts):
    return pl.pallas_call(
        mix_kernel,
        out_shape=VMEM((64, 512), jnp.float32),
        in_specs=whole(4),
        out_specs=whole()[0],
        compiler_params=pltpu.CompilerParams(vmem_limit_bytes=8 * 2**20),
        name="mix",
    )(bias.reshape(64, 1), *parts)


def finish(begun, part):
    return pl.pallas_call(
        finish_kernel,
        out_shape=jax.ShapeDtypeStruct((64, 512), jnp.bfloat16),
        in_specs=whole(2),
        out_specs=whole()[0],
        compiler_params=pltpu.CompilerParams(vmem_limit_bytes=8 * 2**20),
        name="finish",
    )(begun, part)


def piece_table(request, beside, across):
    my_x, my_z, my_core = (lax.axis_index(a) for a in VERT)
    wanted = jnp.concatenate(
        [r[top + 6 : top + 7, :LANES] for r, top in ((request, 0), (beside, 0), (across, 0), (across, 8))], axis=0
    )
    ahead = (wanted >> 1) - my_z
    ahead = jnp.where(my_core == 0, -ahead, ahead) & 7
    same = (wanted & 1) == my_core
    place = jnp.zeros_like(wanted)
    for distance, (ours, theirs) in enumerate(
        ((0, 1), (4, 5), (2, 3), (6, 7), (8, 15), (14, 13), (10, 9), (12, 11))
    ):
        place = jnp.where(ahead == distance, jnp.where(same, ours, theirs), place)
    here = (wanted >= 0) & ((wanted >> 4) == my_x)
    return jnp.where(here, place, -1)


def body(features_t, weight, bias, self_mask, halo_mask, block_src, halo_rows, outside_degree):
    scaled, root, request, held_self, held_halo = head(block_src, self_mask, halo_mask, outside_degree, features_t, halo_rows)

    partner = shifted(scaled, "core", 1)
    both = joined(scaled, partner)
    two = opposed(both, 2)
    four = shifted(scaled, "z", 4)
    one = opposed(joined(both, two), 1)
    beside = paired(request, "x", 1)
    late_request, late_beside, _ = lax.optimization_barrier((request, beside, two))
    across = paired(jnp.concatenate([late_request, late_beside], axis=0), "x", 3)
    table = piece_table(request, beside, across)
    rest = []
    for piece in (two, one, four):
        rest.append(shifted(piece, "core", 1))
    table = placed(table)
    pieces = (scaled, partner, two, one, four, *rest)
    picked = selected((1, 2, 3), table, (beside, across), pieces)
    vals = []
    for at, k in enumerate((1, 3, 2)):
        vals.append(paired(picked[at], "x", k))
    vals += selected((0,), table, (request,), pieces)

    held_halo, held_self, _ = lax.optimization_barrier((held_halo, held_self, picked[0]))
    turned, begun = prepared(held_halo, held_self, scaled)
    weight, bias, _ = lax.optimization_barrier((weight, bias, picked[0]))
    my_af = lax.axis_index("af")
    columns = jnp.stack(
        [
            jnp.pad(lax.dynamic_slice_in_dim(weight, (my_af ^ k) * 64, 64, 1), ((0, 0), (0, 64)))
            for k in range(4)
        ]
    )
    sent = aggregate(vals, turned, begun, root, columns)
    parts = [sent[0]]
    for k in (2, 3, 1):
        parts.append(paired(sent[k], "af", k))
    begun = mix(bias, parts[:3])
    return finish(begun, parts[3])


def solution(mesh):
    finer = Mesh(mesh.devices.reshape(4, 8, 2, 4), ("x", "z", "core", "af"))
    return jax.shard_map(
        body,
        mesh=finer,
        in_specs=(
            P("af", VERT),
            P("af", None),
            P("af"),
            P(VERT, None, None),
            P(VERT, None, None, None),
            P(VERT, None),
            P(VERT, None, None),
            P(VERT),
        ),
        out_specs=P("af", VERT),
        check_vma=False,
    )
```

```python
import functools

import jax
import jax.numpy as jnp
from jax import lax
from jax.experimental import pallas as pl
from jax.experimental.pallas import tpu as pltpu
from jax.sharding import Mesh
from jax.sharding import PartitionSpec as P


VERT = ("x", "z", "core")
LANES = 128
FEATS = 32
SURE = 3
VMEM = pltpu.VMEM


def shifted(array, axis, by):
    count = lax.axis_size(axis)
    return lax.ppermute(array, axis, [(i, (i + by) % count) for i in range(count)])


def paired(array, axis, by):
    return lax.ppermute(array, axis, [(i, i ^ by) for i in range(lax.axis_size(axis))])


def opposed(array, by):
    count = lax.axis_size("z")
    pairs = [(2 * z + c, 2 * ((z + (by, -by)[c]) % count) + c) for z in range(count) for c in range(2)]
    return lax.ppermute(array, ("z", "core"), pairs)


def whole(count=1):
    return [pl.BlockSpec(memory_space=VMEM)] * count


def in_hbm(array):
    return pltpu.with_memory_space_constraint(array, pltpu.HBM)


def head_kernel(
    sources_in, self_in, halo_in, outside_in, features_in, rows_in,
    scaled, root, request, self_out, halo_out,
    sources, self_mask, halo_mask, outside, features, rows, total, small, own, slot,
):
    smalls = [
        pltpu.make_async_copy(src, dst, small.at[k])
        for k, (src, dst) in enumerate(
            (
                (sources_in, sources),
                (outside_in, outside),
                (features_in, features),
                (rows_in, rows),
            )
        )
    ]
    owns = [
        pltpu.make_async_copy(
            self_in.at[0, pl.ds(r * 256, 256), :], self_mask.at[pl.ds(r * 256, 256), :], own.at[r]
        )
        for r in range(2)
    ]
    slots = [pltpu.make_async_copy(halo_in.at[0, s], halo_mask.at[s], slot.at[s]) for s in range(6)]
    smalls[0].start()
    owns[0].start()
    owns[1].start()
    for s in range(SURE):
        slots[s].start()
    for copy in smalls[1:]:
        copy.start()
    smalls[0].wait()
    for s in range(SURE, 6):
        pl.when(sources[0, s] >= 0)(slots[s].start)
    for s in range(1, 6):

        def left_out(s=s):
            halo_out[s] = jnp.zeros_like(halo_out[s])

        pl.when(sources[0, s] < 0)(left_out)
    for copy in smalls[1:]:
        copy.wait()

    for s in range(6):
        for g in range(2):
            request[s : s + 1, g * LANES : (g + 1) * LANES] = rows[2 * s + g]
    lane = lax.broadcasted_iota(jnp.int32, (2, 256), 1)
    listed = jnp.full((2, 256), -1, jnp.int32)
    for s in range(6):
        listed = jnp.where(lane == s, sources[0, s], listed)
    request[6:8, :] = listed

    for r in range(2):
        owns[r].wait()
        at = slice(r * 256, (r + 1) * 256)
        block = self_mask[at, :]
        self_out[at, :] = block.astype(jnp.float32).astype(jnp.bfloat16)
        total[at, :] = (block[:, :128] + block[:, 128:256]) + (block[:, 256:384] + block[:, 384:])
    for s in range(6):

        if s < SURE:
            slots[s].wait()

        def counted(s=s):
            if s >= SURE:
                slots[s].wait()
            block = halo_mask[s]
            halo_out[s] = block.astype(jnp.float32).astype(jnp.bfloat16)
            total[...] += block[:, :LANES] + block[:, LANES:]

        if s:
            pl.when(sources[0, s] >= 0)(counted)
        else:
            counted()
    ones = jnp.ones((8, LANES), jnp.bfloat16)
    counts = total[...].astype(jnp.float32).astype(jnp.bfloat16)
    summed = lax.dot_general(ones, counts, (((1,), (1,)), ((), ())), preferred_element_type=jnp.float32)
    inverse = lax.rsqrt(summed[:1] + 1.0 + outside[...].astype(jnp.float32))
    root[...] = inverse
    scaled[...] = (features[...].astype(jnp.float32) * inverse).astype(jnp.bfloat16)


def head(block_src, self_mask, halo_mask, outside_degree, features_t, halo_rows):
    return pl.pallas_call(
        head_kernel,
        out_shape=[
            VMEM((FEATS, 512), jnp.bfloat16),
            VMEM((1, 512), jnp.float32),
            VMEM((8, 256), jnp.int32),
            VMEM((512, 512), jnp.bfloat16),
            VMEM((6, 512, 256), jnp.bfloat16),
        ],
        in_specs=[pl.BlockSpec(memory_space=pltpu.HBM)] * 6,
        out_specs=whole(5),
        scratch_shapes=[
            pltpu.SMEM((1, 6), jnp.int32),
            VMEM((512, 512), jnp.int32),
            VMEM((6, 512, 256), jnp.int32),
            VMEM((1, 512), jnp.int32),
            VMEM((FEATS, 512), jnp.bfloat16),
            VMEM((12, 1, LANES), jnp.int32),
            VMEM((512, LANES), jnp.int32),
            pltpu.SemaphoreType.DMA((4,)),
            pltpu.SemaphoreType.DMA((2,)),
            pltpu.SemaphoreType.DMA((6,)),
        ],
        compiler_params=pltpu.CompilerParams(vmem_limit_bytes=8 * 2**20),
        name="head",
    )(
        *map(
            in_hbm,
            (
                block_src,
                self_mask,
                halo_mask,
                outside_degree.reshape(1, 512),
                features_t,
                halo_rows.reshape(12, 1, LANES),
            ),
        )
    )


def place_kernel(listed, table, arrived):
    copy = pltpu.make_async_copy(listed, table, arrived)
    copy.start()
    copy.wait()


def placed(listed):
    return pl.pallas_call(
        place_kernel,
        out_shape=pltpu.SMEM((4, LANES), jnp.int32),
        in_specs=whole(),
        out_specs=pl.BlockSpec(memory_space=pltpu.SMEM),
        scratch_shapes=[pltpu.SemaphoreType.DMA],
        compiler_params=pltpu.CompilerParams(vmem_limit_bytes=2**20),
        name="place",
    )(listed)


def select_kernel(dests, table, *refs):
    if dests == (0,):
        requests, refs = ((refs[0], 0),), refs[1:]
    else:
        requests, refs = ((refs[0], 0), (refs[1], 0), (refs[1], 8)), refs[2:]
    pieces, outs, held = refs[: -1 - len(dests)], refs[-1 - len(dests) : -1], refs[-1]
    at = 0
    for piece in pieces:
        for k in range(piece.shape[0] // FEATS):
            held[at] = piece[k * FEATS : (k + 1) * FEATS, :].astype(jnp.float32)
            at += 1
    for dest, (request, top), out in zip(dests, requests, outs):
        out[...] = jnp.zeros_like(out)
        for s in range(6):
            which = table[dest, s]

            @pl.when(which >= 0)
            def _():
                for g in range(2):
                    rows = request[top + s : top + s + 1, g * LANES : (g + 1) * LANES]
                    rows = jnp.broadcast_to(rows, (FEATS, LANES))
                    lane = rows & (LANES - 1)
                    block = rows >> 7
                    picked = jnp.zeros((FEATS, LANES), jnp.float32)
                    for t in range(4):
                        part = held[which, :, t * LANES : (t + 1) * LANES]
                        took = jnp.take_along_axis(part, lane, axis=1, mode="promise_in_bounds")
                        picked = jnp.where(block == t, took, picked)
                    to = s * 256 + g * LANES
                    out[:, to : to + LANES] = picked.astype(jnp.bfloat16)


def selected(dests, table, requests, pieces):
    operands = (*requests, *pieces)
    return pl.pallas_call(
        functools.partial(select_kernel, dests),
        out_shape=[VMEM((FEATS, 1536), jnp.bfloat16)] * len(dests),
        in_specs=[pl.BlockSpec(memory_space=pltpu.SMEM)] + whole(len(operands)),
        out_specs=whole(len(dests)),
        scratch_shapes=[VMEM((16, FEATS, 512), jnp.float32)],
        compiler_params=pltpu.CompilerParams(vmem_limit_bytes=8 * 2**20),
    )(pltpu.with_memory_space_constraint(table, pltpu.SMEM), *operands)


def join_kernel(*refs):
    at = 0
    for piece in refs[:-1]:
        refs[-1][at : at + piece.shape[0], :] = piece[...]
        at += piece.shape[0]


def joined(*pieces):
    return pl.pallas_call(
        join_kernel,
        out_shape=VMEM((sum(p.shape[0] for p in pieces), 512), jnp.bfloat16),
        in_specs=whole(len(pieces)),
        out_specs=whole()[0],
        compiler_params=pltpu.CompilerParams(vmem_limit_bytes=2 * 2**20),
        name="join",
    )(*pieces)


def prepare_kernel(halo_mask, self_mask, scaled, turned, begun):
    for s in range(6):
        turned[s * 256 : (s + 1) * 256, :] = halo_mask[s].T
    begun[...] = scaled[...].astype(jnp.float32) + lax.dot_general(
        scaled[...], self_mask[...], (((1,), (1,)), ((), ())), preferred_element_type=jnp.float32
    )


def prepared(halo_mask, self_mask, scaled):
    return pl.pallas_call(
        prepare_kernel,
        out_shape=[VMEM((1536, 512), jnp.bfloat16), VMEM((FEATS, 512), jnp.float32)],
        in_specs=whole(3),
        out_specs=whole(2),
        compiler_params=pltpu.CompilerParams(vmem_limit_bytes=16 * 2**20),
        name="prepare",
    )(halo_mask, self_mask, scaled)


def aggregate_kernel(mine, one, two, three, turned, begun, root, columns, *outs):
    halo_vals = mine[...] + one[...] + two[...] + three[...]
    summed = begun[...] + jnp.dot(halo_vals, turned[...], preferred_element_type=jnp.float32)
    aggregated = (summed * root[...]).astype(jnp.bfloat16)
    for k in range(4):
        outs[k][:, :512] = aggregated
        outs[k][:, 512:] = columns[k]


def aggregate(vals, turned, begun, root, columns):
    return pl.pallas_call(
        aggregate_kernel,
        out_shape=[VMEM((FEATS, 640), jnp.bfloat16)] * 4,
        in_specs=whole(8),
        out_specs=whole(4),
        compiler_params=pltpu.CompilerParams(vmem_limit_bytes=8 * 2**20),
        name="aggregate",
    )(*vals, turned, begun, root, columns)


def mixed(part):
    return lax.dot_general(
        part[:, 512:576], part[:, :512], (((0,), (0,)), ((), ())), preferred_element_type=jnp.float32
    )


def mix_kernel(bias, one, two, three, out):
    out[...] = bias[...] + mixed(one) + mixed(two) + mixed(three)


def finish_kernel(begun, part, out):
    out[...] = jnp.maximum(begun[...] + mixed(part), 0.0).astype(jnp.bfloat16)


def mix(bias, parts):
    return pl.pallas_call(
        mix_kernel,
        out_shape=VMEM((64, 512), jnp.float32),
        in_specs=whole(4),
        out_specs=whole()[0],
        compiler_params=pltpu.CompilerParams(vmem_limit_bytes=8 * 2**20),
        name="mix",
    )(bias.reshape(64, 1), *parts)


def finish(begun, part):
    return pl.pallas_call(
        finish_kernel,
        out_shape=jax.ShapeDtypeStruct((64, 512), jnp.bfloat16),
        in_specs=whole(2),
        out_specs=whole()[0],
        compiler_params=pltpu.CompilerParams(vmem_limit_bytes=8 * 2**20),
        name="finish",
    )(begun, part)


def piece_table(request, beside, across):
    my_x, my_z, my_core = (lax.axis_index(a) for a in VERT)
    wanted = jnp.concatenate(
        [r[top + 6 : top + 7, :LANES] for r, top in ((request, 0), (beside, 0), (across, 0), (across, 8))], axis=0
    )
    ahead = (wanted >> 1) - my_z
    ahead = jnp.where(my_core == 0, -ahead, ahead) & 7
    same = (wanted & 1) == my_core
    place = jnp.zeros_like(wanted)
    for distance, (ours, theirs) in enumerate(
        ((0, 1), (4, 5), (2, 3), (6, 7), (8, 15), (14, 13), (10, 9), (12, 11))
    ):
        place = jnp.where(ahead == distance, jnp.where(same, ours, theirs), place)
    here = (wanted >= 0) & ((wanted >> 4) == my_x)
    return jnp.where(here, place, -1)


def body(features_t, weight, bias, self_mask, halo_mask, block_src, halo_rows, outside_degree):
    scaled, root, request, held_self, held_halo = head(block_src, self_mask, halo_mask, outside_degree, features_t, halo_rows)

    partner = shifted(scaled, "core", 1)
    both = joined(scaled, partner)
    two = opposed(both, 2)
    four = shifted(scaled, "z", 4)
    one = opposed(joined(both, two), 1)
    beside = paired(request, "x", 1)
    late_request, late_beside, _ = lax.optimization_barrier((request, beside, two))
    across = paired(jnp.concatenate([late_request, late_beside], axis=0), "x", 3)
    table = piece_table(request, beside, across)
    rest = []
    for piece in (two, one, four):
        rest.append(shifted(piece, "core", 1))
    table = placed(table)
    pieces = (scaled, partner, two, one, four, *rest)
    picked = selected((1, 2, 3), table, (beside, across), pieces)
    vals = []
    for at, k in enumerate((1, 3, 2)):
        vals.append(paired(picked[at], "x", k))
    vals += selected((0,), table, (request,), pieces)

    held_halo, held_self, _ = lax.optimization_barrier((held_halo, held_self, picked[0]))
    turned, begun = prepared(held_halo, held_self, scaled)
    weight, bias, _ = lax.optimization_barrier((weight, bias, begun))
    my_af = lax.axis_index("af")
    columns = jnp.stack(
        [
            jnp.pad(lax.dynamic_slice_in_dim(weight, (my_af ^ k) * 64, 64, 1), ((0, 0), (0, 64)))
            for k in range(4)
        ]
    )
    sent = aggregate(vals, turned, begun, root, columns)
    parts = [sent[0]]
    for k in (2, 3, 1):
        parts.append(paired(sent[k], "af", k))
    begun = mix(bias, parts[:3])
    return finish(begun, parts[3])


def solution(mesh):
    finer = Mesh(mesh.devices.reshape(4, 8, 2, 4), ("x", "z", "core", "af"))
    return jax.shard_map(
        body,
        mesh=finer,
        in_specs=(
            P("af", VERT),
            P("af", None),
            P("af"),
            P(VERT, None, None),
            P(VERT, None, None, None),
            P(VERT, None),
            P(VERT, None, None),
            P(VERT),
        ),
        out_specs=P("af", VERT),
        check_vma=False,
    )
```

```python
import functools

import jax
import jax.numpy as jnp
from jax import lax
from jax.experimental import pallas as pl
from jax.experimental.pallas import tpu as pltpu
from jax.sharding import Mesh
from jax.sharding import PartitionSpec as P


VERT = ("x", "z", "core")
LANES = 128
FEATS = 32
SURE = 3
VMEM = pltpu.VMEM


def shifted(array, axis, by):
    count = lax.axis_size(axis)
    return lax.ppermute(array, axis, [(i, (i + by) % count) for i in range(count)])


def paired(array, axis, by):
    return lax.ppermute(array, axis, [(i, i ^ by) for i in range(lax.axis_size(axis))])


def opposed(array, by):
    count = lax.axis_size("z")
    pairs = [(2 * z + c, 2 * ((z + (by, -by)[c]) % count) + c) for z in range(count) for c in range(2)]
    return lax.ppermute(array, ("z", "core"), pairs)


def whole(count=1):
    return [pl.BlockSpec(memory_space=VMEM)] * count


def in_hbm(array):
    return pltpu.with_memory_space_constraint(array, pltpu.HBM)


def head_kernel(
    sources_in, self_in, halo_in, outside_in, features_in, rows_in,
    scaled, root, request, self_out, halo_out,
    sources, self_mask, halo_mask, outside, features, rows, total, small, own, slot,
):
    smalls = [
        pltpu.make_async_copy(src, dst, small.at[k])
        for k, (src, dst) in enumerate(
            (
                (sources_in, sources),
                (outside_in, outside),
                (features_in, features),
                (rows_in, rows),
            )
        )
    ]
    owns = [
        pltpu.make_async_copy(
            self_in.at[0, pl.ds(r * 256, 256), :], self_mask.at[pl.ds(r * 256, 256), :], own.at[r]
        )
        for r in range(2)
    ]
    slots = [pltpu.make_async_copy(halo_in.at[0, s], halo_mask.at[s], slot.at[s]) for s in range(6)]
    smalls[0].start()
    owns[0].start()
    owns[1].start()
    for s in range(SURE):
        slots[s].start()
    for copy in smalls[1:]:
        copy.start()
    smalls[0].wait()
    for s in range(SURE, 6):
        pl.when(sources[0, s] >= 0)(slots[s].start)
    for s in range(1, 6):

        def left_out(s=s):
            halo_out[s] = jnp.zeros_like(halo_out[s])

        pl.when(sources[0, s] < 0)(left_out)
    for copy in smalls[1:]:
        copy.wait()

    for s in range(6):
        for g in range(2):
            request[s : s + 1, g * LANES : (g + 1) * LANES] = rows[2 * s + g]
    lane = lax.broadcasted_iota(jnp.int32, (2, 256), 1)
    listed = jnp.full((2, 256), -1, jnp.int32)
    for s in range(6):
        listed = jnp.where(lane == s, sources[0, s], listed)
    request[6:8, :] = listed

    for r in range(2):
        owns[r].wait()
        at = slice(r * 256, (r + 1) * 256)
        block = self_mask[at, :]
        self_out[at, :] = block.astype(jnp.float32).astype(jnp.bfloat16)
        total[at, :] = (block[:, :128] + block[:, 128:256]) + (block[:, 256:384] + block[:, 384:])
    for s in range(6):

        if s < SURE:
            slots[s].wait()

        def counted(s=s):
            if s >= SURE:
                slots[s].wait()
            block = halo_mask[s]
            halo_out[s] = block.astype(jnp.float32).astype(jnp.bfloat16)
            total[...] += block[:, :LANES] + block[:, LANES:]

        if s:
            pl.when(sources[0, s] >= 0)(counted)
        else:
            counted()
    ones = jnp.ones((8, LANES), jnp.bfloat16)
    counts = total[...].astype(jnp.float32).astype(jnp.bfloat16)
    summed = lax.dot_general(ones, counts, (((1,), (1,)), ((), ())), preferred_element_type=jnp.float32)
    inverse = lax.rsqrt(summed[:1] + 1.0 + outside[...].astype(jnp.float32))
    root[...] = inverse
    scaled[...] = (features[...].astype(jnp.float32) * inverse).astype(jnp.bfloat16)


def head(block_src, self_mask, halo_mask, outside_degree, features_t, halo_rows):
    return pl.pallas_call(
        head_kernel,
        out_shape=[
            VMEM((FEATS, 512), jnp.bfloat16),
            VMEM((1, 512), jnp.float32),
            VMEM((8, 256), jnp.int32),
            VMEM((512, 512), jnp.bfloat16),
            VMEM((6, 512, 256), jnp.bfloat16),
        ],
        in_specs=[pl.BlockSpec(memory_space=pltpu.HBM)] * 6,
        out_specs=whole(5),
        scratch_shapes=[
            pltpu.SMEM((1, 6), jnp.int32),
            VMEM((512, 512), jnp.int32),
            VMEM((6, 512, 256), jnp.int32),
            VMEM((1, 512), jnp.int32),
            VMEM((FEATS, 512), jnp.bfloat16),
            VMEM((12, 1, LANES), jnp.int32),
            VMEM((512, LANES), jnp.int32),
            pltpu.SemaphoreType.DMA((4,)),
            pltpu.SemaphoreType.DMA((2,)),
            pltpu.SemaphoreType.DMA((6,)),
        ],
        compiler_params=pltpu.CompilerParams(vmem_limit_bytes=8 * 2**20),
        name="head",
    )(
        *map(
            in_hbm,
            (
                block_src,
                self_mask,
                halo_mask,
                outside_degree.reshape(1, 512),
                features_t,
                halo_rows.reshape(12, 1, LANES),
            ),
        )
    )


def place_kernel(listed, table, arrived):
    copy = pltpu.make_async_copy(listed, table, arrived)
    copy.start()
    copy.wait()


def placed(listed):
    return pl.pallas_call(
        place_kernel,
        out_shape=pltpu.SMEM((4, LANES), jnp.int32),
        in_specs=whole(),
        out_specs=pl.BlockSpec(memory_space=pltpu.SMEM),
        scratch_shapes=[pltpu.SemaphoreType.DMA],
        compiler_params=pltpu.CompilerParams(vmem_limit_bytes=2**20),
        name="place",
    )(listed)


def select_kernel(dests, table, *refs):
    if dests == (0,):
        requests, refs = ((refs[0], 0),), refs[1:]
    else:
        requests, refs = ((refs[0], 0), (refs[1], 0), (refs[1], 8)), refs[2:]
    pieces, outs, held = refs[: -1 - len(dests)], refs[-1 - len(dests) : -1], refs[-1]
    at = 0
    for piece in pieces:
        for k in range(piece.shape[0] // FEATS):
            held[at] = piece[k * FEATS : (k + 1) * FEATS, :]
            at += 1
    for dest, (request, top), out in zip(dests, requests, outs):
        out[...] = jnp.zeros_like(out)
        for s in range(6):
            which = table[dest, s]

            @pl.when(which >= 0)
            def _():
                for g in range(2):
                    rows = request[top + s : top + s + 1, g * LANES : (g + 1) * LANES]
                    rows = jnp.broadcast_to(rows, (FEATS, LANES))
                    lane = rows & (LANES - 1)
                    block = rows >> 7
                    picked = jnp.zeros((FEATS, LANES), jnp.float32)
                    for t in range(4):
                        part = held[which, :, t * LANES : (t + 1) * LANES].astype(jnp.float32)
                        took = jnp.take_along_axis(part, lane, axis=1, mode="promise_in_bounds")
                        picked = jnp.where(block == t, took, picked)
                    to = s * 256 + g * LANES
                    out[:, to : to + LANES] = picked.astype(jnp.bfloat16)


def selected(dests, table, requests, pieces):
    operands = (*requests, *pieces)
    return pl.pallas_call(
        functools.partial(select_kernel, dests),
        out_shape=[VMEM((FEATS, 1536), jnp.bfloat16)] * len(dests),
        in_specs=[pl.BlockSpec(memory_space=pltpu.SMEM)] + whole(len(operands)),
        out_specs=whole(len(dests)),
        scratch_shapes=[VMEM((16, FEATS, 512), jnp.bfloat16)],
        compiler_params=pltpu.CompilerParams(vmem_limit_bytes=8 * 2**20),
    )(pltpu.with_memory_space_constraint(table, pltpu.SMEM), *operands)


def join_kernel(*refs):
    at = 0
    for piece in refs[:-1]:
        refs[-1][at : at + piece.shape[0], :] = piece[...]
        at += piece.shape[0]


def joined(*pieces):
    return pl.pallas_call(
        join_kernel,
        out_shape=VMEM((sum(p.shape[0] for p in pieces), 512), jnp.bfloat16),
        in_specs=whole(len(pieces)),
        out_specs=whole()[0],
        compiler_params=pltpu.CompilerParams(vmem_limit_bytes=2 * 2**20),
        name="join",
    )(*pieces)


def prepare_kernel(halo_mask, self_mask, scaled, turned, begun):
    for s in range(6):
        turned[s * 256 : (s + 1) * 256, :] = halo_mask[s].T
    begun[...] = scaled[...].astype(jnp.float32) + lax.dot_general(
        scaled[...], self_mask[...], (((1,), (1,)), ((), ())), preferred_element_type=jnp.float32
    )


def prepared(halo_mask, self_mask, scaled):
    return pl.pallas_call(
        prepare_kernel,
        out_shape=[VMEM((1536, 512), jnp.bfloat16), VMEM((FEATS, 512), jnp.float32)],
        in_specs=whole(3),
        out_specs=whole(2),
        compiler_params=pltpu.CompilerParams(vmem_limit_bytes=16 * 2**20),
        name="prepare",
    )(halo_mask, self_mask, scaled)


def aggregate_kernel(mine, one, two, three, turned, begun, root, columns, *outs):
    halo_vals = mine[...] + one[...] + two[...] + three[...]
    summed = begun[...] + jnp.dot(halo_vals, turned[...], preferred_element_type=jnp.float32)
    aggregated = (summed * root[...]).astype(jnp.bfloat16)
    for k in range(4):
        outs[k][:, :512] = aggregated
        outs[k][:, 512:] = columns[k]


def aggregate(vals, turned, begun, root, columns):
    return pl.pallas_call(
        aggregate_kernel,
        out_shape=[VMEM((FEATS, 640), jnp.bfloat16)] * 4,
        in_specs=whole(8),
        out_specs=whole(4),
        compiler_params=pltpu.CompilerParams(vmem_limit_bytes=8 * 2**20),
        name="aggregate",
    )(*vals, turned, begun, root, columns)


def mixed(part):
    return lax.dot_general(
        part[:, 512:576], part[:, :512], (((0,), (0,)), ((), ())), preferred_element_type=jnp.float32
    )


def mix_kernel(bias, one, two, three, out):
    out[...] = bias[...] + mixed(one) + mixed(two) + mixed(three)


def finish_kernel(begun, part, out):
    out[...] = jnp.maximum(begun[...] + mixed(part), 0.0).astype(jnp.bfloat16)


def mix(bias, parts):
    return pl.pallas_call(
        mix_kernel,
        out_shape=VMEM((64, 512), jnp.float32),
        in_specs=whole(4),
        out_specs=whole()[0],
        compiler_params=pltpu.CompilerParams(vmem_limit_bytes=8 * 2**20),
        name="mix",
    )(bias.reshape(64, 1), *parts)


def finish(begun, part):
    return pl.pallas_call(
        finish_kernel,
        out_shape=jax.ShapeDtypeStruct((64, 512), jnp.bfloat16),
        in_specs=whole(2),
        out_specs=whole()[0],
        compiler_params=pltpu.CompilerParams(vmem_limit_bytes=8 * 2**20),
        name="finish",
    )(begun, part)


def piece_table(request, beside, across):
    my_x, my_z, my_core = (lax.axis_index(a) for a in VERT)
    wanted = jnp.concatenate(
        [r[top + 6 : top + 7, :LANES] for r, top in ((request, 0), (beside, 0), (across, 0), (across, 8))], axis=0
    )
    ahead = (wanted >> 1) - my_z
    ahead = jnp.where(my_core == 0, -ahead, ahead) & 7
    same = (wanted & 1) == my_core
    place = jnp.zeros_like(wanted)
    for distance, (ours, theirs) in enumerate(
        ((0, 1), (4, 5), (2, 3), (6, 7), (8, 11), (15, 14), (10, 9), (13, 12))
    ):
        place = jnp.where(ahead == distance, jnp.where(same, ours, theirs), place)
    here = (wanted >= 0) & ((wanted >> 4) == my_x)
    return jnp.where(here, place, -1)


def body(features_t, weight, bias, self_mask, halo_mask, block_src, halo_rows, outside_degree):
    scaled, root, request, held_self, held_halo = head(block_src, self_mask, halo_mask, outside_degree, features_t, halo_rows)

    partner = shifted(scaled, "core", 1)
    both = joined(scaled, partner)
    two = opposed(both, 2)
    four = shifted(scaled, "z", 4)
    one = opposed(joined(both, two), 1)
    beside = paired(request, "x", 1)
    late_request, late_beside, _ = lax.optimization_barrier((request, beside, two))
    across = paired(jnp.concatenate([late_request, late_beside], axis=0), "x", 3)
    table = piece_table(request, beside, across)
    rest = []
    for piece in (joined(two, four), one):
        rest.append(shifted(piece, "core", 1))
    table = placed(table)
    pieces = (scaled, partner, two, one, four, *rest)
    picked = selected((1, 2, 3), table, (beside, across), pieces)
    vals = []
    for at, k in enumerate((1, 3, 2)):
        vals.append(paired(picked[at], "x", k))
    vals += selected((0,), table, (request,), pieces)

    held_halo, held_self, _ = lax.optimization_barrier((held_halo, held_self, picked[0]))
    turned, begun = prepared(held_halo, held_self, scaled)
    weight, bias, _ = lax.optimization_barrier((weight, bias, begun))
    my_af = lax.axis_index("af")
    columns = jnp.stack(
        [
            jnp.pad(lax.dynamic_slice_in_dim(weight, (my_af ^ k) * 64, 64, 1), ((0, 0), (0, 64)))
            for k in range(4)
        ]
    )
    sent = aggregate(vals, turned, begun, root, columns)
    parts = [sent[0]]
    for k in (2, 3, 1):
        parts.append(paired(sent[k], "af", k))
    begun = mix(bias, parts[:3])
    return finish(begun, parts[3])


def solution(mesh):
    finer = Mesh(mesh.devices.reshape(4, 8, 2, 4), ("x", "z", "core", "af"))
    return jax.shard_map(
        body,
        mesh=finer,
        in_specs=(
            P("af", VERT),
            P("af", None),
            P("af"),
            P(VERT, None, None),
            P(VERT, None, None, None),
            P(VERT, None),
            P(VERT, None, None),
            P(VERT),
        ),
        out_specs=P("af", VERT),
        check_vma=False,
    )
```
